32 devices in a mesh: col: 4 (over y, x), row: 8 (over z, core).
Axes of the slice: x: 2, y: 2, z: 4, core: 2. Of those that a mesh axis runs over, the one named last changes fastest.
Arguments:
- data: bfloat16 [16384, 8192], P('row', 'col'), may hold values from -6 to 6
- column_scale: float32 [8192], P('col'), may hold values from 0.25 to 4
- keep_mask: int32 [16384, 8192], P('row', 'col'), may hold values 0 or 1
Outputs:
- band: float32 [8192, 3, 2048], P('col', None, 'row')
The draws below stay inside these ranges and needn't reach their ends.
All inputs are finite; a program needn't handle non-finite values. No bound on the sum of `keep_mask` on one device may be relied on, other than what follows from the above.
Results may differ from the reference program's by a relative error of at most 0.0012.
Values may be sent and summed in bfloat16 or wider, within the bound.
A program may use at most 128 MiB of HBM per device.

```python
import math
import jax
import jax.numpy as jnp
from jax import lax

COLS = 8192
ROWS = 16384
PANEL = 2048
HALF = 3
N_COL = 4


def with_ends(values, key, low, top_value):
    shape = values.shape
    index_at = [jax.random.randint(jax.random.fold_in(key, axis), (), 0, shape[axis]) for axis in range(len(shape))]
    values = values.at[tuple(index_at)].set(low)
    longest = shape.index(max(shape))
    index_at[longest] = (index_at[longest] + 1) % shape[longest]
    return values.at[tuple(index_at)].set(top_value)


def levels(key, shape, shards, least, top_value):
    level, own = 1.0, jax.random.fold_in(key, 6)
    for dim, blocks in shards:
        steps = jnp.exp(jax.random.uniform(jax.random.fold_in(own, dim), (blocks,), jnp.float32, least / len(shards), top_value / len(shards)))
        level = level * jnp.repeat(steps, shape[dim] // blocks).reshape([-1 if axis == dim else 1 for axis in range(len(shape))])
    return level


def normal_values(key, dims, deviation, reach, cuts=(), held_as=jnp.bfloat16):
    drawn = jax.random.normal(key, dims, jnp.float32) * deviation
    if len(cuts) > 0:
        drawn = levels(key, dims, cuts, -0.22, 0.18) * drawn
    return jnp.clip(drawn, min=-reach, max=reach).astype(held_as)


def setup_inputs(seed: int = 0) -> dict:
    splits = jax.random.split(jax.random.key(seed), 4)
    data = normal_values(splits[0], (ROWS, COLS), 1.0, 6.0, ((0, 8), (1, 4)))
    column_scale = jnp.clip(jnp.exp(math.log(4.0) - 2.7725887 * jax.random.uniform(splits[1], (COLS,), jnp.float32) ** levels(splits[1], (COLS,), ((0, 4),), -0.2, 0.2)), 0.25, 4.0)
    keep_mask = with_ends((jax.random.randint(splits[2], (ROWS, COLS), 0, 4) < 3).astype(jnp.int32), jax.random.fold_in(splits[2], 1), 0, 1)
    return {"data": data, "column_scale": column_scale, "keep_mask": keep_mask}


def reference(data, column_scale, keep_mask):
    values = data.astype(jnp.float32) * column_scale[None, :]
    colsq = lax.optimization_barrier(jnp.sum(values * values, axis=0))
    divisor = jnp.minimum(jnp.sqrt(colsq + 1.0), jnp.sqrt(jnp.float32(ROWS)))
    scaled = (keep_mask.astype(jnp.float32) * values / divisor[None, :]).astype(jnp.bfloat16)
    wide = scaled.astype(jnp.float32)
    blocks = []
    for panel_index in range(N_COL):
        left = wide[:, panel_index * PANEL:(panel_index + 1) * PANEL]
        rolled = jnp.roll(wide, -panel_index * PANEL, axis=1)[:, :HALF * PANEL]
        tile = jnp.dot(left.T, rolled, precision=lax.Precision.HIGHEST, preferred_element_type=jnp.float32)
        blocks.append(tile.reshape(PANEL, HALF, PANEL))
    return jnp.concatenate(blocks, axis=0)
```

```python
import functools

import jax
import jax.numpy as jnp
from jax import lax
from jax.experimental import pallas as pl
from jax.experimental.pallas import tpu as pltpu
from jax.experimental.layout import Layout, with_layout_constraint
from jax.sharding import PartitionSpec as P


CHUNKS = 2
TOP = 16384.0


def passed_along(block, axis, distance):
    size = lax.axis_size(axis)
    return lax.ppermute(block, axis, [((i - distance) % size, i) for i in range(size)])


def swapped(block, axis):
    return lax.ppermute(block, axis, [(i, i ^ 1) for i in range(lax.axis_size(axis))])


def product(left, right):
    return lax.dot_general(
        left, right, (((0,), (0,)), ((), ())), preferred_element_type=jnp.float32
    )


def chunk_of(block, owners, q):
    width = block.shape[-1] // (owners * CHUNKS)
    starts = [(owner * CHUNKS + q) * width for owner in range(owners)]
    return jnp.concatenate([block[..., s:s + width] for s in starts], axis=-1)


def summed_over_rows(partial, pairs):
    me = lax.axis_index("row")
    pair, half = me // 2, me % 2
    parts = partial.reshape((pairs, 2, -1) + partial.shape[1:])
    mine = lax.dynamic_index_in_dim(parts, half, 1, keepdims=False)
    theirs = lax.dynamic_index_in_dim(parts, 1 - half, 1, keepdims=False)
    from_partner = swapped(theirs, "row")

    def both(at):
        one, two = (
            lax.dynamic_index_in_dim(a, at % pairs, 0, keepdims=False).astype(jnp.float32)
            for a in (mine, from_partner)
        )
        return one + two

    total = both(pair)
    plain = Layout(major_to_minor=(0, 1))
    blocks = [
        with_layout_constraint(both(pair + step).astype(jnp.float16), plain)
        for step in range(1, pairs)
    ]
    for step, block in enumerate(blocks, 1):
        arrived = with_layout_constraint(passed_along(block, "row", 2 * step), plain)
        total = total + arrived.astype(jnp.float32)
    return total, blocks


def on_device(data, column_scale, keep_mask):
    rows = lax.axis_size("row")
    n_col = lax.axis_size("col")
    offsets = n_col // 2 + 1
    values = data.astype(jnp.float32) * column_scale[None, :]
    colsq = lax.psum(jnp.sum(values * values, axis=0), "row")
    total_rows = data.shape[0] * rows
    divisor = jnp.minimum(jnp.sqrt(colsq + 1.0), jnp.sqrt(jnp.float32(total_rows)))
    norm = jnp.sqrt(jnp.maximum(colsq, 1e-30)) / divisor
    norms = [norm] + [passed_along(norm, "col", -offset) for offset in range(1, offsets)]
    divisor, norms = lax.optimization_barrier((divisor, norms))
    scaled = (keep_mask.astype(jnp.float32) * values / divisor[None, :]).astype(jnp.bfloat16)
    even = lax.axis_index("col") % 2 == 0

    own = [chunk_of(scaled, rows, q) for q in range(CHUNKS)]
    panels = {(0, q): own[q] for q in range(CHUNKS)}
    for q in range(CHUNKS):
        for offset in range(2, offsets, 2):
            panels[offset, q] = passed_along(own[q], "col", -offset)
    gain = TOP / norm
    kept = {}

    def stage(name, panel, length):
        partial = product(panel, scaled) * gain[None, :] * (1.0 / length)[:, None]
        partial = partial.astype(jnp.float16)
        total, blocks = summed_over_rows(partial, rows // 2)
        back = length.reshape(rows, -1)[lax.axis_index("row")]
        kept[name] = total * (norm * (1.0 / TOP))[None, :] * back[:, None]
        return blocks

    blocks = stage("0", scaled, norm)
    for offset in list(range(2, offsets, 2)) + list(range(1, offsets, 2)):
        for q in range(CHUNKS):
            if offset % 2:
                if n_col % 2 == 0 and (offset + 1, q) in panels:
                    after, before = panels[offset + 1, q], panels[offset - 1, q]
                    panels[offset, q] = swapped(jnp.where(even, after, before), "col")
                else:
                    panels[offset, q] = passed_along(own[q], "col", -offset)
            panels[offset, q], blocks = lax.optimization_barrier((panels[offset, q], blocks))
            length = chunk_of(norms[offset], rows, q)
            blocks = stage(f"{offset}_{q}", panels[offset, q], length)
    result = [kept["0"]]
    for offset in range(1, offsets):
        result.append(jnp.concatenate([kept[f"{offset}_{q}"] for q in range(CHUNKS)], axis=0))
    return jnp.stack([total.T for total in result], axis=1)


LANES = 128
SENT_TOP = 1024.0
MESH_ID = pl.DeviceIdType.MESH


def sent(x):
    x = x * jnp.abs(x)
    return (x * jnp.abs(x)).astype(jnp.bfloat16)


def received(y):
    y = y.astype(jnp.float32)
    size = lax.rsqrt(lax.rsqrt(jnp.maximum(jnp.abs(y), 1e-37)))
    return jnp.where(y < 0.0, -size, size)


def square_kernel(
    n_row, data, scale, mask, out,
    buf, own_t, chunk, swap_out, swap_in, hold, near, far, line, masks, sums, plain, vec, back,
    data_sem, mask_sem, sum_send, sum_recv, vec_send, vec_recv, y_send, y_recv, x_send, x_recv,
    swap_send, swap_recv, line_send, near_recv, far_recv, out_sem, near_free,
):
    c, r = lax.axis_index("col"), lax.axis_index("row")
    z, k = r // 2, r % 2
    rows, panel = data.shape
    pairs = n_row // 2
    piece = panel // n_row
    wide = 2 * LANES
    parts = piece // LANES
    chunks = pairs * parts
    block = rows // 4
    half = rows // 2
    last = 3 * chunks + 2
    near_slots, hold_slots, line_slots = 3 * pairs, 7, 4
    forwards = c % 2 == 0
    y_peer, x_peer = (c + 2) % 4, c + 1 - 2 * (c % 2)
    partner = 2 * (z + 1 - 2 * (z % 2)) + k
    inner = jnp.logical_or(z == 1, z == 2)

    def target_of(q):
        at = q % pairs
        return jnp.where(at == 0, 0, jnp.where(at == 1, 3, at - 1))

    def column_of(q, core):
        start = (2 * target_of(q) + core) * piece + (q // pairs) * LANES
        return pl.multiple_of(start, LANES)

    def stage_of(m):
        offset = m % 3
        return offset, m // 3 - jnp.where(offset == 1, 1, 0)

    def valid(m):
        return (m >= 0) & (m < last) & (m != 1) & (m != last - 2)

    def role_of(q):
        goal = target_of(q)
        same = z // 2 == goal // 2
        return jnp.where(z == goal, 3, jnp.where(same, 1, jnp.where(inner, 2, 1)))

    def data_copy(q, side):
        return pltpu.make_async_copy(
            data.at[:, pl.ds(column_of(q, k if side == 0 else 1 - k), LANES)],
            buf.at[0, q, :, pl.ds(side * LANES, LANES)], data_sem.at[q, side])

    def mask_copy(q, side):
        return pltpu.make_async_copy(
            mask.at[:, pl.ds(column_of(q, k if side == 0 else 1 - k), LANES)],
            masks.at[q % 2, :, pl.ds(side * LANES, LANES)], mask_sem.at[q % 2, side])

    def half_of(offset, q, part):
        return buf.at[offset, q, pl.ds(part * half, half), :]

    def y_copy(q, part):
        return pltpu.make_async_remote_copy(
            half_of(0, q, part), half_of(2, q, part), y_send.at[q, part], y_recv.at[q, part],
            device_id=(y_peer, r), device_id_type=MESH_ID)

    def x_copy(q, part, source):
        return pltpu.make_async_remote_copy(
            half_of(source, q, part), half_of(1, q, part), x_send.at[q, part], x_recv.at[q, part],
            device_id=(x_peer, r), device_id_type=MESH_ID)

    def start_own(q):
        for part in range(2):
            y_copy(q, part).start()

            @pl.when(jnp.logical_not(forwards))
            def _():
                x_copy(q, part, 0).start()

    @pl.loop(0, chunks)
    def _(q):
        for side in range(2):
            data_copy(q, side).start()

    for q in range(2):
        for side in range(2):
            mask_copy(q, side).start()

    barrier = pltpu.get_barrier_semaphore()
    for step in range(1, n_row):
        pl.semaphore_signal(barrier, inc=1, device_id=(c, (r + step) % n_row), device_id_type=MESH_ID)
    for step in range(1, 4):
        pl.semaphore_signal(barrier, inc=1, device_id=((c + step) % 4, r), device_id_type=MESH_ID)
    pl.semaphore_wait(barrier, n_row + 2)

    @pl.loop(0, chunks)
    def _(q):
        for side in range(2):
            data_copy(q, side).wait()
            mask_copy(q, side).wait()
        scales = jnp.concatenate(
            [scale[:, pl.ds(column_of(q, k), LANES)], scale[:, pl.ds(column_of(q, 1 - k), LANES)]], axis=1)
        step = 128

        def read(b, total):
            at = pl.ds(pl.multiple_of(b * step, step), step)
            values = buf[0, q, at, :].astype(jnp.float32)
            kept = masks[q % 2, at, :].astype(jnp.float32) * values
            buf[0, q, at, :] = kept.astype(jnp.bfloat16)
            values = values * scales
            return total + jnp.sum((values * values).reshape(step // 8, 8, wide), axis=0)

        total = lax.fori_loop(0, rows // step, read, jnp.zeros((8, wide), jnp.float32))
        total = jnp.sum(total, axis=0, keepdims=True)
        sums[r, :, pl.ds(column_of(q, k), LANES)] = total[:, :LANES]
        sums[r, :, pl.ds(column_of(q, 1 - k), LANES)] = total[:, LANES:]

        @pl.when(q + 2 < chunks)
        def _():
            for side in range(2):
                mask_copy(q + 2, side).start()

        @pl.when(q == 0)
        def _():
            start_own(q)

    def sum_copy(step):
        peer = (r + step) % n_row
        return pltpu.make_async_remote_copy(
            sums.at[r], sums.at[r], sum_send.at[step], sum_recv.at[step],
            device_id=(c, peer), device_id_type=MESH_ID)

    def sum_arrival(step):
        origin = (r + n_row - step) % n_row
        return pltpu.make_async_remote_copy(
            sums.at[origin], sums.at[origin], sum_send.at[step], sum_recv.at[step],
            device_id=(c, origin), device_id_type=MESH_ID)

    for step in range(1, n_row):
        sum_copy(step).start()
    for step in range(1, n_row):
        sum_arrival(step).wait_recv()
    colsq = sums[0]
    for origin in range(1, n_row):
        colsq = colsq + sums[origin]
    divisor = jnp.minimum(jnp.sqrt(colsq + 1.0), jnp.sqrt(jnp.full_like(colsq, rows * n_row)))
    size = jnp.sqrt(jnp.maximum(colsq, 1e-30)) / divisor
    up = jnp.full_like(size, SENT_TOP)
    down = jnp.full_like(size, 1.0 / SENT_TOP)
    for power in (32, 16, 8, 4, 2, 1):
        small = size < 2.0 ** -power
        size = jnp.where(small, size * 2.0 ** power, size)
        up = jnp.where(small, up * 2.0 ** power, up)
        down = jnp.where(small, down * 2.0 ** -power, down)
    plain[0:1, :] = scale[...] / divisor * up
    plain[1:2, :] = down

    @pl.loop(0, chunks)
    def _(q):
        for side in range(2):
            column = column_of(q, k if side == 0 else 1 - k)
            to = pl.ds(pl.multiple_of(q * wide + side * LANES, LANES), LANES)
            vec[0, :, to] = plain[:, pl.ds(column, LANES)]

    def vec_copy(offset):
        return pltpu.make_async_remote_copy(
            vec.at[0], vec.at[offset], vec_send.at[offset], vec_recv.at[offset],
            device_id=((c + 4 - offset) % 4, r), device_id_type=MESH_ID)

    for offset in (2, 1):
        vec_copy(offset).start()

    @pl.loop(1, chunks)
    def _(q):
        start_own(q)

    @pl.loop(0, chunks)
    def _(q):
        for side in range(2):
            column = column_of(q, k if side == 0 else 1 - k)
            lanes = pl.ds(side * LANES, LANES)
            factors = vec[0, :, pl.ds(pl.multiple_of(q * wide + side * LANES, LANES), LANES)]

            @pl.loop(0, rows // block)
            def _(b):
                at = pl.ds(pl.multiple_of(b * block, block), block)
                scaled = (buf[0, q, at, lanes].astype(jnp.float32) * factors[0:1, :]).astype(jnp.bfloat16)
                own_t[pl.ds(column, LANES), at] = scaled.T

            back[pl.ds(column, LANES), :] = jnp.broadcast_to(factors[1:2, :], (LANES, LANES)).T

    for offset in (2, 1):
        vec_copy(offset).wait_recv()

    tall = panel // 4

    def swap_copy(m):
        return pltpu.make_async_remote_copy(
            swap_out.at[m % 2], swap_in.at[m % 4], swap_send.at[m % 2], swap_recv.at[m % 4],
            device_id=(c, 2 * z + 1 - k), device_id_type=MESH_ID)

    def near_copy(m):
        return pltpu.make_async_remote_copy(
            line.at[m % line_slots], near.at[m % near_slots],
            line_send.at[m % line_slots], near_recv.at[m % near_slots],
            device_id=(c, partner), device_id_type=MESH_ID)

    def far_copy(m, offset, q):
        slot = offset * parts + q // pairs
        return pltpu.make_async_remote_copy(
            line.at[m % line_slots], far.at[slot], line_send.at[m % line_slots], far_recv.at[slot],
            device_id=(c, 2 * target_of(q) + k), device_id_type=MESH_ID)

    def out_copy(m, offset, q):
        lanes = pl.ds(pl.multiple_of((q // pairs) * LANES, LANES), LANES)
        return pltpu.make_async_copy(
            hold.at[m % hold_slots], out.at[offset, :, lanes], out_sem.at[m % hold_slots])

    def give_back(m):
        @pl.when(valid(m + near_slots))
        def _():
            pl.semaphore_signal(
                near_free.at[m % near_slots], inc=1, device_id=(c, partner), device_id_type=MESH_ID)

    def in_blocks(body):
        step = 256

        @pl.loop(0, panel // step)
        def _(b):
            body(pl.ds(pl.multiple_of(b * step, step), step))

    @pl.loop(0, last + hold_slots)
    def _(n):
        def settle(m, action):
            offset, q = stage_of(m)

            @pl.when(valid(m))
            def _():
                action(offset, q)

        def close_swap(offset, q):
            swap_copy(n - 2).wait_send()

        def close_out(offset, q):
            @pl.when(role_of(q) == 3)
            def _():
                out_copy(n - hold_slots, offset, q).wait()

        settle(n - 2, close_swap)
        settle(n - hold_slots, close_out)

        def arrive(part):
            q = n // 3
            y_copy(q, part).wait_recv()

            @pl.when(forwards)
            def _():
                x_copy(q, part, 2).start()

        @pl.when((n % 3 == 1) & (n // 3 < chunks))
        def _():
            arrive(0)

        @pl.when((n % 3 == 2) & (n // 3 < chunks))
        def _():
            arrive(1)

        def multiply(offset, q):
            @pl.when(offset == 1)
            def _():
                for part in range(2):
                    x_copy(q, part, 0).wait_recv()

            factors = vec[offset, 0:1, pl.ds(pl.multiple_of(q * wide, wide), wide)]

            @pl.loop(0, rows // block)
            def _(b):
                at = pl.ds(pl.multiple_of(b * block, block), block)
                chunk[at, :] = (buf[offset, q, at, :].astype(jnp.float32) * factors).astype(jnp.bfloat16)

            @pl.loop(0, panel // tall)
            def _(b):
                at = pl.ds(pl.multiple_of(b * tall, tall), tall)
                product = jnp.dot(own_t[at, :], chunk[...], preferred_element_type=jnp.float32)
                hold[n % hold_slots, at, :] = product[:, :LANES]
                swap_out[n % 2, at, :] = product[:, LANES:]

            swap_copy(n).start()

        settle(n, multiply)

        def join(offset, q):
            m = n - 1
            swap_copy(m).wait_recv()
            role = role_of(q)

            @pl.when(role == 1)
            def _():
                def body(at):
                    line[m % line_slots, at, :] = sent(hold[m % hold_slots, at, :] + swap_in[m % 4, at, :])

                in_blocks(body)

                @pl.when(valid(m - near_slots))
                def _():
                    pl.semaphore_wait(near_free.at[m % near_slots], 1)

                near_copy(m).start()

            @pl.when(role != 1)
            def _():
                def body(at):
                    hold[m % hold_slots, at, :] = hold[m % hold_slots, at, :] + swap_in[m % 4, at, :]

                in_blocks(body)

        def close_line(offset, q):
            @pl.when(role_of(q) != 3)
            def _():
                near_copy(n - 1 - line_slots).wait_send()

        settle(n - 1 - line_slots, close_line)
        settle(n - 1, join)

        def relay(offset, q):
            m = n - 3

            @pl.when(role_of(q) == 2)
            def _():
                near_copy(m).wait_recv()

                def body(at):
                    line[m % line_slots, at, :] = sent(
                        hold[m % hold_slots, at, :] + received(near[m % near_slots, at, :]))

                in_blocks(body)
                give_back(m)
                far_copy(m, offset, q).start()

        settle(n - 3, relay)

        def finish(offset, q):
            m = n - 5

            @pl.when(role_of(q) == 3)
            def _():
                near_copy(m).wait_recv()
                far_copy(m, offset, q).wait_recv()
                slot = offset * parts + q // pairs
                factors = vec[offset, 1:2, pl.ds(pl.multiple_of(q * wide, wide), LANES)]

                def body(at):
                    total = hold[m % hold_slots, at, :] + received(near[m % near_slots, at, :])
                    total = total + received(far[slot, at, :])
                    hold[m % hold_slots, at, :] = total * back[at, :] * factors

                in_blocks(body)
                give_back(m)
                out_copy(m, offset, q).start()

        settle(n - 5, finish)

    @pl.loop(0, chunks)
    def _(q):
        for part in range(2):
            y_copy(q, part).wait_send()
            x_copy(q, part, 0).wait_send()

    for step in range(1, n_row):
        sum_copy(step).wait_send()
    for offset in (2, 1):
        vec_copy(offset).wait_send()


def square_program(n_row):
    def on_device(data, column_scale, keep_mask):
        rows, panel = data.shape
        piece = panel // n_row
        pairs, parts = n_row // 2, piece // LANES
        chunks = pairs * parts
        f32, bf16, dma = jnp.float32, jnp.bfloat16, pltpu.SemaphoreType.DMA
        band = pl.pallas_call(
            functools.partial(square_kernel, n_row),
            out_shape=jax.ShapeDtypeStruct((3, panel, piece), f32),
            in_specs=[pl.BlockSpec(memory_space=pl.ANY), pl.BlockSpec(memory_space=pltpu.VMEM),
                      pl.BlockSpec(memory_space=pl.ANY)],
            out_specs=pl.BlockSpec(memory_space=pl.ANY),
            scratch_shapes=[
                pltpu.VMEM((3, chunks, rows, 2 * LANES), bf16),
                pltpu.VMEM((panel, rows), bf16),
                pltpu.VMEM((rows, 2 * LANES), bf16),
                pltpu.VMEM((2, panel, LANES), f32),
                pltpu.VMEM((4, panel, LANES), f32),
                pltpu.VMEM((7, panel, LANES), f32),
                pltpu.VMEM((3 * pairs, panel, LANES), bf16),
                pltpu.VMEM((3 * parts, panel, LANES), bf16),
                pltpu.VMEM((4, panel, LANES), bf16),
                pltpu.VMEM((2, rows, 2 * LANES), jnp.int32),
                pltpu.VMEM((n_row, 1, panel), f32),
                pltpu.VMEM((8, panel), f32),
                pltpu.VMEM((3, 8, panel), f32),
                pltpu.VMEM((panel, LANES), f32),
                dma((chunks, 2)), dma((2, 2)), dma((n_row,)), dma((n_row,)), dma((3,)), dma((3,)),
                dma((chunks, 2)), dma((chunks, 2)), dma((chunks, 2)), dma((chunks, 2)),
                dma((2,)), dma((4,)), dma((4,)), dma((3 * pairs,)), dma((3 * parts,)), dma((7,)),
                pltpu.SemaphoreType.REGULAR((3 * pairs,)),
            ],
            compiler_params=pltpu.CompilerParams(
                collective_id=0, has_side_effects=True, vmem_limit_bytes=67_043_328),
        )(data, column_scale[None, :], keep_mask)
        return band.transpose(1, 0, 2)

    return on_device


def solution(mesh):
    in_specs = (P("row", "col"), P("col"), P("row", "col"))
    out_specs = P("col", None, "row")

    def mapped(body):
        return jax.shard_map(
            body, mesh=mesh, in_specs=in_specs, out_specs=out_specs, check_vma=False
        )

    if mesh.shape["col"] == 4 and mesh.shape["row"] == 8:
        return mapped(square_program(mesh.shape["row"]))
    return mapped(on_device)
```

```python
import functools

import jax
import jax.numpy as jnp
from jax import lax
from jax.experimental import pallas as pl
from jax.experimental.pallas import tpu as pltpu
from jax.experimental.layout import Layout, with_layout_constraint
from jax.sharding import PartitionSpec as P


CHUNKS = 2
TOP = 16384.0


def passed_along(block, axis, distance):
    size = lax.axis_size(axis)
    return lax.ppermute(block, axis, [((i - distance) % size, i) for i in range(size)])


def swapped(block, axis):
    return lax.ppermute(block, axis, [(i, i ^ 1) for i in range(lax.axis_size(axis))])


def product(left, right):
    return lax.dot_general(
        left, right, (((0,), (0,)), ((), ())), preferred_element_type=jnp.float32
    )


def chunk_of(block, owners, q):
    width = block.shape[-1] // (owners * CHUNKS)
    starts = [(owner * CHUNKS + q) * width for owner in range(owners)]
    return jnp.concatenate([block[..., s:s + width] for s in starts], axis=-1)


def summed_over_rows(partial, pairs):
    me = lax.axis_index("row")
    pair, half = me // 2, me % 2
    parts = partial.reshape((pairs, 2, -1) + partial.shape[1:])
    mine = lax.dynamic_index_in_dim(parts, half, 1, keepdims=False)
    theirs = lax.dynamic_index_in_dim(parts, 1 - half, 1, keepdims=False)
    from_partner = swapped(theirs, "row")

    def both(at):
        one, two = (
            lax.dynamic_index_in_dim(a, at % pairs, 0, keepdims=False).astype(jnp.float32)
            for a in (mine, from_partner)
        )
        return one + two

    total = both(pair)
    plain = Layout(major_to_minor=(0, 1))
    blocks = [
        with_layout_constraint(both(pair + step).astype(jnp.float16), plain)
        for step in range(1, pairs)
    ]
    for step, block in enumerate(blocks, 1):
        arrived = with_layout_constraint(passed_along(block, "row", 2 * step), plain)
        total = total + arrived.astype(jnp.float32)
    return total, blocks


def on_device(data, column_scale, keep_mask):
    rows = lax.axis_size("row")
    n_col = lax.axis_size("col")
    offsets = n_col // 2 + 1
    values = data.astype(jnp.float32) * column_scale[None, :]
    colsq = lax.psum(jnp.sum(values * values, axis=0), "row")
    total_rows = data.shape[0] * rows
    divisor = jnp.minimum(jnp.sqrt(colsq + 1.0), jnp.sqrt(jnp.float32(total_rows)))
    norm = jnp.sqrt(jnp.maximum(colsq, 1e-30)) / divisor
    norms = [norm] + [passed_along(norm, "col", -offset) for offset in range(1, offsets)]
    divisor, norms = lax.optimization_barrier((divisor, norms))
    scaled = (keep_mask.astype(jnp.float32) * values / divisor[None, :]).astype(jnp.bfloat16)
    even = lax.axis_index("col") % 2 == 0

    own = [chunk_of(scaled, rows, q) for q in range(CHUNKS)]
    panels = {(0, q): own[q] for q in range(CHUNKS)}
    for q in range(CHUNKS):
        for offset in range(2, offsets, 2):
            panels[offset, q] = passed_along(own[q], "col", -offset)
    gain = TOP / norm
    kept = {}

    def stage(name, panel, length):
        partial = product(panel, scaled) * gain[None, :] * (1.0 / length)[:, None]
        partial = partial.astype(jnp.float16)
        total, blocks = summed_over_rows(partial, rows // 2)
        back = length.reshape(rows, -1)[lax.axis_index("row")]
        kept[name] = total * (norm * (1.0 / TOP))[None, :] * back[:, None]
        return blocks

    blocks = stage("0", scaled, norm)
    for offset in list(range(2, offsets, 2)) + list(range(1, offsets, 2)):
        for q in range(CHUNKS):
            if offset % 2:
                if n_col % 2 == 0 and (offset + 1, q) in panels:
                    after, before = panels[offset + 1, q], panels[offset - 1, q]
                    panels[offset, q] = swapped(jnp.where(even, after, before), "col")
                else:
                    panels[offset, q] = passed_along(own[q], "col", -offset)
            panels[offset, q], blocks = lax.optimization_barrier((panels[offset, q], blocks))
            length = chunk_of(norms[offset], rows, q)
            blocks = stage(f"{offset}_{q}", panels[offset, q], length)
    result = [kept["0"]]
    for offset in range(1, offsets):
        result.append(jnp.concatenate([kept[f"{offset}_{q}"] for q in range(CHUNKS)], axis=0))
    return jnp.stack([total.T for total in result], axis=1)


LANES = 128
SENT_TOP = 1024.0
MESH_ID = pl.DeviceIdType.MESH


def sent(x):
    x = x * jnp.abs(x)
    return (x * jnp.abs(x)).astype(jnp.bfloat16)


def received(y):
    y = y.astype(jnp.float32)
    size = lax.rsqrt(lax.rsqrt(jnp.maximum(jnp.abs(y), 1e-37)))
    return jnp.where(y < 0.0, -size, size)


def square_kernel(
    n_row, data, scale, mask, out,
    buf, own_t, chunk, swap_out, swap_in, hold, near, far, line, turned, mirror, stage, masks, sums, plain, vec, back,
    data_sem, mask_sem, sum_send, sum_recv, vec_send, vec_recv, y_send, y_recv, x_send, x_recv,
    swap_send, swap_recv, line_send, near_recv, far_recv, turn_send, turn_recv, out_sem, stage_sem, near_free,
):
    c, r = lax.axis_index("col"), lax.axis_index("row")
    z, k = r // 2, r % 2
    rows, panel = data.shape
    pairs = n_row // 2
    piece = panel // n_row
    wide = 2 * LANES
    parts = piece // LANES
    chunks = pairs * parts
    block = rows // 4
    half = rows // 2
    last = 3 * chunks + 2
    near_slots, hold_slots, line_slots, swap_slots = 3 * pairs, 6, 4, 3
    tall = panel // pairs
    forwards = c % 2 == 0
    y_peer, x_peer = (c + 2) % 4, c + 1 - 2 * (c % 2)
    partner = 2 * (z + 1 - 2 * (z % 2)) + k
    inner = jnp.logical_or(z == 1, z == 2)

    def target_of(q):
        at = q % pairs
        return jnp.where(at == 0, 0, jnp.where(at == 1, 3, at - 1))

    def column_of(q, core):
        start = (2 * target_of(q) + core) * piece + (q // pairs) * LANES
        return pl.multiple_of(start, LANES)

    def stage_of(m):
        offset, turn = m % 3, m // 3
        ahead = jnp.where(m == 1, 1, (turn + 2) % chunks)
        own = jnp.logical_or(m == 1, offset == 0)
        return jnp.where(own, 0, offset), jnp.where(own, ahead, turn - jnp.where(offset == 1, 1, 0))

    def valid(m):
        return (m >= 0) & (m < last) & (m != last - 5) & (m != last - 2)

    def near_slot(m):
        return jnp.where(m == 1, near_slots, m % near_slots)

    def blocks_of(offset, q):
        return jnp.where(offset == 0, target_of(q) + 1, pairs)

    def rows_of(g):
        return pl.ds(pl.multiple_of(g * tall, tall), tall)

    def role_of(q):
        goal = target_of(q)
        same = z // 2 == goal // 2
        return jnp.where(z == goal, 3, jnp.where(same, 1, jnp.where(inner, 2, 1)))

    def strip_of(u):
        q, side = u // 2, u % 2
        to = pl.ds(pl.multiple_of(side * LANES, LANES), LANES)
        return q, to, pl.ds(column_of(q, k + side - 2 * k * side), LANES)

    def data_copy(u):
        q, to, columns = strip_of(u)
        return pltpu.make_async_copy(data.at[:, columns], buf.at[0, q, :, to], data_sem.at[u])

    def mask_copy(u):
        _, _, columns = strip_of(u)
        return pltpu.make_async_copy(mask.at[:, columns], masks.at[u % 2], mask_sem.at[u % 2])

    def half_of(offset, q, part):
        return buf.at[offset, q, pl.ds(part * half, half), :]

    def y_copy(q, part):
        return pltpu.make_async_remote_copy(
            half_of(0, q, part), half_of(2, q, part), y_send.at[q, part], y_recv.at[q, part],
            device_id=(y_peer, r), device_id_type=MESH_ID)

    def x_copy(q, part, source):
        return pltpu.make_async_remote_copy(
            half_of(source, q, part), half_of(1, q, part), x_send.at[q, part], x_recv.at[q, part],
            device_id=(x_peer, r), device_id_type=MESH_ID)

    def start_own(q):
        for part in range(2):
            y_copy(q, part).start()

            @pl.when(jnp.logical_not(forwards))
            def _():
                x_copy(q, part, 0).start()

    mask_copy(0).start()
    mask_copy(1).start()

    @pl.loop(0, 2 * chunks)
    def _(u):
        data_copy(u).start()

    barrier = pltpu.get_barrier_semaphore()
    for step in range(1, n_row):
        pl.semaphore_signal(barrier, inc=1, device_id=(c, (r + step) % n_row), device_id_type=MESH_ID)
    for step in range(1, 4):
        pl.semaphore_signal(barrier, inc=1, device_id=((c + step) % 4, r), device_id_type=MESH_ID)
    pl.semaphore_wait(barrier, n_row + 2)

    @pl.loop(0, 2 * chunks)
    def _(u):
        data_copy(u).wait()
        mask_copy(u).wait()
        q, to, columns = strip_of(u)
        scales = scale[:, columns]
        step = 256

        def read(b, total):
            at = pl.ds(pl.multiple_of(b * step, step), step)
            values = buf[0, q, at, to].astype(jnp.float32)
            kept = masks[u % 2, at, :].astype(jnp.float32) * values
            buf[0, q, at, to] = kept.astype(jnp.bfloat16)
            values = values * scales
            return total + jnp.sum((values * values).reshape(step // 8, 8, LANES), axis=0)

        total = lax.fori_loop(0, rows // step, read, jnp.zeros((8, LANES), jnp.float32))
        sums[r, :, columns] = jnp.sum(total, axis=0, keepdims=True)

        @pl.when(u + 2 < 2 * chunks)
        def _():
            mask_copy(u + 2).start()

        @pl.when(u == 1)
        def _():
            start_own(0)

    def sum_copy(step):
        peer = (r + step) % n_row
        return pltpu.make_async_remote_copy(
            sums.at[r], sums.at[r], sum_send.at[step], sum_recv.at[step],
            device_id=(c, peer), device_id_type=MESH_ID)

    def sum_arrival(step):
        origin = (r + n_row - step) % n_row
        return pltpu.make_async_remote_copy(
            sums.at[origin], sums.at[origin], sum_send.at[step], sum_recv.at[step],
            device_id=(c, origin), device_id_type=MESH_ID)

    for step in range(1, n_row):
        sum_copy(step).start()
    for step in range(1, n_row):
        sum_arrival(step).wait_recv()
    colsq = sums[0]
    for origin in range(1, n_row):
        colsq = colsq + sums[origin]
    divisor = jnp.minimum(jnp.sqrt(colsq + 1.0), jnp.sqrt(jnp.full_like(colsq, rows * n_row)))
    size = jnp.sqrt(jnp.maximum(colsq, 1e-30)) / divisor
    up = jnp.full_like(size, SENT_TOP)
    down = jnp.full_like(size, 1.0 / SENT_TOP)
    for power in (32, 16, 8, 4, 2, 1):
        small = size < 2.0 ** -power
        size = jnp.where(small, size * 2.0 ** power, size)
        up = jnp.where(small, up * 2.0 ** power, up)
        down = jnp.where(small, down * 2.0 ** -power, down)
    plain[0:1, :] = scale[...] / divisor * up
    plain[1:2, :] = down

    @pl.loop(0, chunks)
    def _(q):
        for side in range(2):
            column = column_of(q, k if side == 0 else 1 - k)
            to = pl.ds(pl.multiple_of(q * wide + side * LANES, LANES), LANES)
            vec[0, :, to] = plain[:, pl.ds(column, LANES)]

    def vec_copy(offset):
        return pltpu.make_async_remote_copy(
            vec.at[0], vec.at[offset], vec_send.at[offset], vec_recv.at[offset],
            device_id=((c + 4 - offset) % 4, r), device_id_type=MESH_ID)

    for offset in (2, 1):
        vec_copy(offset).start()

    @pl.loop(1, chunks)
    def _(q):
        start_own(q)

    @pl.loop(0, chunks)
    def _(q):
        for side in range(2):
            column = column_of(q, k if side == 0 else 1 - k)
            lanes = pl.ds(side * LANES, LANES)
            factors = vec[0, :, pl.ds(pl.multiple_of(q * wide + side * LANES, LANES), LANES)]

            @pl.loop(0, rows // block)
            def _(b):
                at = pl.ds(pl.multiple_of(b * block, block), block)
                scaled = (buf[0, q, at, lanes].astype(jnp.float32) * factors[0:1, :]).astype(jnp.bfloat16)
                own_t[pl.ds(column, LANES), at] = scaled.T

            back[pl.ds(column, LANES), :] = jnp.broadcast_to(factors[1:2, :], (LANES, LANES)).T

    def swap_copy(m, g):
        return pltpu.make_async_remote_copy(
            swap_out.at[m % 2, rows_of(g)], swap_in.at[m % swap_slots, rows_of(g)],
            swap_send.at[m % 2, g], swap_recv.at[m % swap_slots, g],
            device_id=(c, 2 * z + 1 - k), device_id_type=MESH_ID)

    def near_copy(m, g):
        return pltpu.make_async_remote_copy(
            line.at[m % line_slots, rows_of(g)], near.at[near_slot(m), rows_of(g)],
            line_send.at[m % line_slots, g], near_recv.at[near_slot(m), g],
            device_id=(c, partner), device_id_type=MESH_ID)

    def far_copy(m, offset, q, g):
        slot = offset * parts + q // pairs
        return pltpu.make_async_remote_copy(
            line.at[m % line_slots, rows_of(g)], far.at[slot, rows_of(g)],
            line_send.at[m % line_slots, g], far_recv.at[slot, g],
            device_id=(c, 2 * target_of(q) + k), device_id_type=MESH_ID)

    def out_copy(m, offset, q, g):
        lanes = pl.ds(pl.multiple_of((q // pairs) * LANES, LANES), LANES)
        return pltpu.make_async_copy(
            hold.at[m % hold_slots, rows_of(g)], out.at[offset, rows_of(g), lanes],
            out_sem.at[m % hold_slots, g])

    def turn_copy(part, g, core):
        return pltpu.make_async_remote_copy(
            turned.at[part, g, core], mirror.at[z - 1, k, part],
            turn_send.at[part, g, core], turn_recv.at[z - 1, k, part],
            device_id=(c, 2 * g + core), device_id_type=MESH_ID)

    def turn_arrival(goal, core, part):
        return pltpu.make_async_remote_copy(
            turned.at[0, 0, 0], mirror.at[goal - 1, core, part],
            turn_send.at[0, 0, 0], turn_recv.at[goal - 1, core, part],
            device_id=(c, 2 * goal + core), device_id_type=MESH_ID)

    def stage_copy(e, start):
        return pltpu.make_async_copy(
            stage.at[e % 2], out.at[0, pl.ds(start, LANES), :], stage_sem.at[e % 2])

    def mirrored(e):
        goal, core, part = e // (2 * parts) + 1, (e // parts) % 2, e % parts
        start = pl.multiple_of((2 * goal + core) * piece + part * LANES, LANES)
        return goal, core, part, start

    @pl.loop(0, last + hold_slots)
    def _(n):
        def settle(m, action):
            offset, q = stage_of(m)

            @pl.when(valid(m))
            def _():
                @pl.loop(0, blocks_of(offset, q))
                def _(g):
                    action(offset, q, g)

        def close_swap(offset, q, g):
            swap_copy(n - 2, g).wait_send()

        def close_out(offset, q, g):
            @pl.when(role_of(q) == 3)
            def _():
                out_copy(n - hold_slots, offset, q, g).wait()

        def close_line(offset, q, g):
            @pl.when(role_of(q) != 3)
            def _():
                near_copy(n - 1 - line_slots, g).wait_send()

        settle(n - 2, close_swap)
        settle(n - hold_slots, close_out)

        def arrive(part):
            q = n // 3
            y_copy(q, part).wait_recv()

            @pl.when(forwards)
            def _():
                x_copy(q, part, 2).start()

        @pl.when((n % 3 == 1) & (n // 3 < chunks))
        def _():
            arrive(0)

        @pl.when((n % 3 == 2) & (n // 3 < chunks))
        def _():
            arrive(1)

        @pl.when(n == 2)
        def _():
            vec_copy(2).wait_recv()

        @pl.when(n == 4)
        def _():
            vec_copy(1).wait_recv()

        @pl.when(valid(n))
        def _():
            offset, q = stage_of(n)

            @pl.when(offset == 1)
            def _():
                for part in range(2):
                    x_copy(q, part, 0).wait_recv()

            factors = vec[offset, 0:1, pl.ds(pl.multiple_of(q * wide, wide), wide)]

            @pl.loop(0, rows // block)
            def _(b):
                at = pl.ds(pl.multiple_of(b * block, block), block)
                chunk[at, :] = (buf[offset, q, at, :].astype(jnp.float32) * factors).astype(jnp.bfloat16)

        settle(n - 1 - line_slots, close_line)

        def join(offset, q, g):
            m = n - 1
            at = rows_of(g)
            role = role_of(q)
            swap_copy(m, g).wait_recv()

            @pl.when(role == 1)
            def _():
                line[m % line_slots, at, :] = sent(hold[m % hold_slots, at, :] + swap_in[m % swap_slots, at, :])

                @pl.when((g == 0) & (m >= near_slots) & valid(m - near_slots) & (m != near_slots + 1))
                def _():
                    pl.semaphore_wait(near_free.at[m % near_slots], 1)

                near_copy(m, g).start()

            @pl.when(role != 1)
            def _():
                hold[m % hold_slots, at, :] = hold[m % hold_slots, at, :] + swap_in[m % swap_slots, at, :]

        settle(n - 1, join)

        def multiply(offset, q, g):
            at = rows_of(g)
            product = jnp.dot(own_t[at, :], chunk[...], preferred_element_type=jnp.float32)
            hold[n % hold_slots, at, :] = product[:, :LANES]
            swap_out[n % 2, at, :] = product[:, LANES:]
            swap_copy(n, g).start()

        settle(n, multiply)

        def give_back(m, offset, q, g):
            @pl.when((g == blocks_of(offset, q) - 1) & valid(m + near_slots) & (m != 1))
            def _():
                pl.semaphore_signal(
                    near_free.at[m % near_slots], inc=1, device_id=(c, partner), device_id_type=MESH_ID)

        def relay(offset, q, g):
            m = n - 3
            at = rows_of(g)

            @pl.when(role_of(q) == 2)
            def _():
                near_copy(m, g).wait_recv()
                line[m % line_slots, at, :] = sent(
                    hold[m % hold_slots, at, :] + received(near[near_slot(m), at, :]))
                give_back(m, offset, q, g)
                far_copy(m, offset, q, g).start()

        settle(n - 3, relay)

        def finish(offset, q, g):
            m = n - 5
            at = rows_of(g)

            @pl.when(role_of(q) == 3)
            def _():
                near_copy(m, g).wait_recv()
                far_copy(m, offset, q, g).wait_recv()
                part = q // pairs
                factors = vec[offset, 1:2, pl.ds(pl.multiple_of(q * wide, wide), LANES)]
                total = hold[m % hold_slots, at, :] + received(near[near_slot(m), at, :])
                total = total + received(far[offset * parts + part, at, :])
                hold[m % hold_slots, at, :] = total * back[at, :] * factors
                give_back(m, offset, q, g)
                out_copy(m, offset, q, g).start()

                @pl.when((offset == 0) & (g < z))
                def _():
                    across = sent(total).T
                    for core in range(2):
                        turned[part, g, core] = across[:, core * piece:(core + 1) * piece]
                        turn_copy(part, g, core).start()

        settle(n - 5, finish)

        @pl.when(n == last + 1)
        def _():
            factors = plain[1:2, pl.ds(pl.multiple_of(r * piece, piece), piece)]

            @pl.loop(2 * parts * z, 2 * parts * (pairs - 1))
            def _(e):
                goal, core, part, start = mirrored(e)
                turn_arrival(goal, core, part).wait_recv()

                @pl.when(e >= 2 * parts * z + 2)
                def _():
                    stage_copy(e - 2, mirrored(e - 2)[3]).wait()

                sizes = back[pl.ds(start, LANES), :]
                sizes = jnp.concatenate([sizes] * (piece // LANES), axis=1)
                stage[e % 2] = received(mirror[goal - 1, core, part]) * sizes * factors
                stage_copy(e, start).start()

    @pl.when(z < pairs - 1)
    def _():
        for e in range(2 * parts * (pairs - 1) - 2, 2 * parts * (pairs - 1)):
            stage_copy(e, mirrored(e)[3]).wait()

    @pl.loop(0, z)
    def _(g):
        for part in range(parts):
            for core in range(2):
                turn_copy(part, g, core).wait_send()

    @pl.loop(0, chunks)
    def _(q):
        for part in range(2):
            y_copy(q, part).wait_send()
            x_copy(q, part, 0).wait_send()

    for step in range(1, n_row):
        sum_copy(step).wait_send()
    for offset in (2, 1):
        vec_copy(offset).wait_send()


def square_program(n_row):
    def on_device(data, column_scale, keep_mask):
        rows, panel = data.shape
        piece = panel // n_row
        pairs, parts = n_row // 2, piece // LANES
        chunks = pairs * parts
        f32, bf16, dma = jnp.float32, jnp.bfloat16, pltpu.SemaphoreType.DMA
        band = pl.pallas_call(
            functools.partial(square_kernel, n_row),
            out_shape=jax.ShapeDtypeStruct((3, panel, piece), f32),
            in_specs=[pl.BlockSpec(memory_space=pl.ANY), pl.BlockSpec(memory_space=pltpu.VMEM),
                      pl.BlockSpec(memory_space=pl.ANY)],
            out_specs=pl.BlockSpec(memory_space=pl.ANY),
            scratch_shapes=[
                pltpu.VMEM((3, chunks, rows, 2 * LANES), bf16),
                pltpu.VMEM((panel, rows), bf16),
                pltpu.VMEM((rows, 2 * LANES), bf16),
                pltpu.VMEM((2, panel, LANES), f32),
                pltpu.VMEM((3, panel, LANES), f32),
                pltpu.VMEM((6, panel, LANES), f32),
                pltpu.VMEM((3 * pairs + 1, panel, LANES), bf16),
                pltpu.VMEM((3 * parts, panel, LANES), bf16),
                pltpu.VMEM((4, panel, LANES), bf16),
                pltpu.VMEM((parts, pairs - 1, 2, LANES, piece), bf16),
                pltpu.VMEM((pairs - 1, 2, parts, LANES, piece), bf16),
                pltpu.VMEM((2, LANES, piece), f32),
                pltpu.VMEM((2, rows, LANES), jnp.int32),
                pltpu.VMEM((n_row, 1, panel), f32),
                pltpu.VMEM((8, panel), f32),
                pltpu.VMEM((3, 8, panel), f32),
                pltpu.VMEM((panel, LANES), f32),
                dma((2 * chunks,)), dma((2,)), dma((n_row,)), dma((n_row,)), dma((3,)), dma((3,)),
                dma((chunks, 2)), dma((chunks, 2)), dma((chunks, 2)), dma((chunks, 2)),
                dma((2, pairs)), dma((3, pairs)), dma((4, pairs)), dma((3 * pairs + 1, pairs)),
                dma((3 * parts, pairs)), dma((parts, pairs - 1, 2)), dma((pairs - 1, 2, parts)),
                dma((6, pairs)), dma((2,)), pltpu.SemaphoreType.REGULAR((3 * pairs,)),
            ],
            compiler_params=pltpu.CompilerParams(
                collective_id=0, has_side_effects=True, vmem_limit_bytes=67_043_328),
        )(data, column_scale[None, :], keep_mask)
        return band.transpose(1, 0, 2)

    return on_device


def solution(mesh):
    in_specs = (P("row", "col"), P("col"), P("row", "col"))
    out_specs = P("col", None, "row")

    def mapped(body):
        return jax.shard_map(
            body, mesh=mesh, in_specs=in_specs, out_specs=out_specs, check_vma=False
        )

    if mesh.shape["col"] == 4 and mesh.shape["row"] == 8:
        return mapped(square_program(mesh.shape["row"]))
    return mapped(on_device)
```

```python
import functools

import jax
import jax.numpy as jnp
from jax import lax
from jax.experimental import pallas as pl
from jax.experimental.pallas import tpu as pltpu
from jax.experimental.layout import Layout, with_layout_constraint
from jax.sharding import PartitionSpec as P


CHUNKS = 2
TOP = 16384.0


def passed_along(block, axis, distance):
    size = lax.axis_size(axis)
    return lax.ppermute(block, axis, [((i - distance) % size, i) for i in range(size)])


def swapped(block, axis):
    return lax.ppermute(block, axis, [(i, i ^ 1) for i in range(lax.axis_size(axis))])


def product(left, right):
    return lax.dot_general(
        left, right, (((0,), (0,)), ((), ())), preferred_element_type=jnp.float32
    )


def chunk_of(block, owners, q):
    width = block.shape[-1] // (owners * CHUNKS)
    starts = [(owner * CHUNKS + q) * width for owner in range(owners)]
    return jnp.concatenate([block[..., s:s + width] for s in starts], axis=-1)


def summed_over_rows(partial, pairs):
    me = lax.axis_index("row")
    pair, half = me // 2, me % 2
    parts = partial.reshape((pairs, 2, -1) + partial.shape[1:])
    mine = lax.dynamic_index_in_dim(parts, half, 1, keepdims=False)
    theirs = lax.dynamic_index_in_dim(parts, 1 - half, 1, keepdims=False)
    from_partner = swapped(theirs, "row")

    def both(at):
        one, two = (
            lax.dynamic_index_in_dim(a, at % pairs, 0, keepdims=False).astype(jnp.float32)
            for a in (mine, from_partner)
        )
        return one + two

    total = both(pair)
    plain = Layout(major_to_minor=(0, 1))
    blocks = [
        with_layout_constraint(both(pair + step).astype(jnp.float16), plain)
        for step in range(1, pairs)
    ]
    for step, block in enumerate(blocks, 1):
        arrived = with_layout_constraint(passed_along(block, "row", 2 * step), plain)
        total = total + arrived.astype(jnp.float32)
    return total, blocks


def on_device(data, column_scale, keep_mask):
    rows = lax.axis_size("row")
    n_col = lax.axis_size("col")
    offsets = n_col // 2 + 1
    values = data.astype(jnp.float32) * column_scale[None, :]
    colsq = lax.psum(jnp.sum(values * values, axis=0), "row")
    total_rows = data.shape[0] * rows
    divisor = jnp.minimum(jnp.sqrt(colsq + 1.0), jnp.sqrt(jnp.float32(total_rows)))
    norm = jnp.sqrt(jnp.maximum(colsq, 1e-30)) / divisor
    norms = [norm] + [passed_along(norm, "col", -offset) for offset in range(1, offsets)]
    divisor, norms = lax.optimization_barrier((divisor, norms))
    scaled = (keep_mask.astype(jnp.float32) * values / divisor[None, :]).astype(jnp.bfloat16)
    even = lax.axis_index("col") % 2 == 0

    own = [chunk_of(scaled, rows, q) for q in range(CHUNKS)]
    panels = {(0, q): own[q] for q in range(CHUNKS)}
    for q in range(CHUNKS):
        for offset in range(2, offsets, 2):
            panels[offset, q] = passed_along(own[q], "col", -offset)
    gain = TOP / norm
    kept = {}

    def stage(name, panel, length):
        partial = product(panel, scaled) * gain[None, :] * (1.0 / length)[:, None]
        partial = partial.astype(jnp.float16)
        total, blocks = summed_over_rows(partial, rows // 2)
        back = length.reshape(rows, -1)[lax.axis_index("row")]
        kept[name] = total * (norm * (1.0 / TOP))[None, :] * back[:, None]
        return blocks

    blocks = stage("0", scaled, norm)
    for offset in list(range(2, offsets, 2)) + list(range(1, offsets, 2)):
        for q in range(CHUNKS):
            if offset % 2:
                if n_col % 2 == 0 and (offset + 1, q) in panels:
                    after, before = panels[offset + 1, q], panels[offset - 1, q]
                    panels[offset, q] = swapped(jnp.where(even, after, before), "col")
                else:
                    panels[offset, q] = passed_along(own[q], "col", -offset)
            panels[offset, q], blocks = lax.optimization_barrier((panels[offset, q], blocks))
            length = chunk_of(norms[offset], rows, q)
            blocks = stage(f"{offset}_{q}", panels[offset, q], length)
    result = [kept["0"]]
    for offset in range(1, offsets):
        result.append(jnp.concatenate([kept[f"{offset}_{q}"] for q in range(CHUNKS)], axis=0))
    return jnp.stack([total.T for total in result], axis=1)


LANES = 128
SENT_TOP = 1024.0
MESH_ID = pl.DeviceIdType.MESH


def sent(x):
    x = x * jnp.abs(x)
    return (x * jnp.abs(x)).astype(jnp.bfloat16)


def received(y):
    y = y.astype(jnp.float32)
    size = lax.rsqrt(lax.rsqrt(jnp.maximum(jnp.abs(y), 1e-37)))
    return jnp.where(y < 0.0, -size, size)


def square_kernel(
    n_row, data, scale, mask, out,
    buf, own_t, chunk, swap_out, swap_in, hold, near, far, line, turned, mirror, stage, masks, sums, plain, vec, back,
    data_sem, mask_sem, sum_send, sum_recv, vec_send, vec_recv, y_send, y_recv, x_send, x_recv,
    swap_send, swap_recv, line_send, near_recv, far_recv, turn_send, turn_recv, out_sem, stage_sem, near_free,
):
    c, r = lax.axis_index("col"), lax.axis_index("row")
    z, k = r // 2, r % 2
    rows, panel = data.shape
    pairs = n_row // 2
    piece = panel // n_row
    wide = 2 * LANES
    parts = piece // LANES
    chunks = pairs * parts
    block = rows // 4
    pieces = 4
    cut = rows // pieces
    last = 3 * chunks + 2
    near_slots, hold_slots, line_slots, swap_slots = 3 * pairs, 7, 5, 3
    tall = panel // pairs
    forwards = c % 2 == 0
    y_peer, x_peer = (c + 2) % 4, c + 1 - 2 * (c % 2)
    partner = 2 * (z + 1 - 2 * (z % 2)) + k
    inner = jnp.logical_or(z == 1, z == 2)

    def target_of(q):
        at = q % pairs
        return jnp.where(at == 0, 0, jnp.where(at == 1, 3, jnp.where(at == 2, 2, 1)))

    def column_of(q, core):
        start = (2 * target_of(q) + core) * piece + (q // pairs) * LANES
        return pl.multiple_of(start, LANES)

    def stage_of(m):
        offset, turn = m % 3, m // 3
        ahead = jnp.where(m == 1, 0, (turn + 1) % chunks)
        own = jnp.logical_or(m == 1, offset == 0)
        return jnp.where(own, 0, offset), jnp.where(own, ahead, turn - jnp.where(offset == 1, 1, 0))

    def valid(m):
        return (m >= 0) & (m < last) & (m != last - 5) & (m != last - 2)

    def near_slot(m):
        return jnp.where(m == 1, near_slots, m % near_slots)

    def blocks_of(offset, q):
        return jnp.where(offset == 0, target_of(q) + 1, pairs)

    def rows_of(g):
        return pl.ds(pl.multiple_of(g * tall, tall), tall)

    def role_of(q):
        goal = target_of(q)
        same = z // 2 == goal // 2
        return jnp.where(z == goal, 3, jnp.where(same, 1, jnp.where(inner, 2, 1)))

    ahead = 3

    def strip_of(u):
        q, side = u // 2, u % 2
        to = pl.ds(pl.multiple_of(side * LANES, LANES), LANES)
        return q, to, pl.ds(column_of(q, k + side - 2 * k * side), LANES)

    def data_copy(u):
        q, to, columns = strip_of(u)
        return pltpu.make_async_copy(data.at[:, columns], buf.at[0, q, :, to], data_sem.at[u])

    def mask_copy(u):
        _, _, columns = strip_of(u)
        return pltpu.make_async_copy(mask.at[:, columns], masks.at[u % ahead], mask_sem.at[u % ahead])

    def cut_of(offset, q, part):
        return buf.at[offset, q, pl.ds(part * cut, cut), :]

    def y_copy(q, part):
        return pltpu.make_async_remote_copy(
            cut_of(0, q, part), cut_of(2, q, part), y_send.at[q, part], y_recv.at[q, part],
            device_id=(y_peer, r), device_id_type=MESH_ID)

    def x_copy(q, part, source):
        return pltpu.make_async_remote_copy(
            cut_of(source, q, part), cut_of(1, q, part), x_send.at[q, part], x_recv.at[q, part],
            device_id=(x_peer, r), device_id_type=MESH_ID)

    def start_own(q):
        for part in range(pieces):
            y_copy(q, part).start()

            @pl.when(jnp.logical_not(forwards))
            def _():
                x_copy(q, part, 0).start()

    for u in range(ahead):
        data_copy(u).start()
        mask_copy(u).start()

    @pl.loop(ahead, 2 * chunks)
    def _(u):
        data_copy(u).start()

    barrier = pltpu.get_barrier_semaphore()
    for step in range(1, n_row):
        pl.semaphore_signal(barrier, inc=1, device_id=(c, (r + step) % n_row), device_id_type=MESH_ID)
    for step in range(1, 4):
        pl.semaphore_signal(barrier, inc=1, device_id=((c + step) % 4, r), device_id_type=MESH_ID)
    pl.semaphore_wait(barrier, n_row + 2)

    @pl.loop(0, 2 * chunks)
    def _(u):
        data_copy(u).wait()
        mask_copy(u).wait()
        q, to, columns = strip_of(u)
        step = 256

        def read(b, total):
            at = pl.ds(pl.multiple_of(b * step, step), step)
            values = buf[0, q, at, to].astype(jnp.float32)
            kept = masks[u % ahead, at, :].astype(jnp.float32) * values
            buf[0, q, at, to] = kept.astype(jnp.bfloat16)
            return total + jnp.sum((values * values).reshape(step // 8, 8, LANES), axis=0)

        total = lax.fori_loop(0, rows // step, read, jnp.zeros((8, LANES), jnp.float32))
        scales = scale[:, columns]
        sums[r, :, columns] = jnp.sum(total, axis=0, keepdims=True) * scales * scales

        @pl.when(u + ahead < 2 * chunks)
        def _():
            mask_copy(u + ahead).start()

        @pl.when(u == 1)
        def _():
            start_own(0)

    def sum_copy(step):
        peer = (r + step) % n_row
        return pltpu.make_async_remote_copy(
            sums.at[r], sums.at[r], sum_send.at[step], sum_recv.at[step],
            device_id=(c, peer), device_id_type=MESH_ID)

    def sum_arrival(step):
        origin = (r + n_row - step) % n_row
        return pltpu.make_async_remote_copy(
            sums.at[origin], sums.at[origin], sum_send.at[step], sum_recv.at[step],
            device_id=(c, origin), device_id_type=MESH_ID)

    for step in range(1, n_row):
        sum_copy(step).start()
    for step in range(1, n_row):
        sum_arrival(step).wait_recv()
    colsq = sums[0]
    for origin in range(1, n_row):
        colsq = colsq + sums[origin]
    divisor = jnp.minimum(jnp.sqrt(colsq + 1.0), jnp.sqrt(jnp.full_like(colsq, rows * n_row)))
    size = jnp.sqrt(jnp.maximum(colsq, 1e-30)) / divisor
    up = jnp.full_like(size, SENT_TOP)
    down = jnp.full_like(size, 1.0 / SENT_TOP)
    for power in (32, 16, 8, 4, 2, 1):
        small = size < 2.0 ** -power
        size = jnp.where(small, size * 2.0 ** power, size)
        up = jnp.where(small, up * 2.0 ** power, up)
        down = jnp.where(small, down * 2.0 ** -power, down)
    plain[0:1, :] = scale[...] / divisor * up
    plain[1:2, :] = down

    @pl.loop(0, chunks)
    def _(q):
        for side in range(2):
            column = column_of(q, k if side == 0 else 1 - k)
            to = pl.ds(pl.multiple_of(q * wide + side * LANES, LANES), LANES)
            vec[0, :, to] = plain[:, pl.ds(column, LANES)]

    def vec_copy(offset):
        return pltpu.make_async_remote_copy(
            vec.at[0], vec.at[offset], vec_send.at[offset], vec_recv.at[offset],
            device_id=((c + 4 - offset) % 4, r), device_id_type=MESH_ID)

    for offset in (2, 1):
        vec_copy(offset).start()

    @pl.loop(1, chunks)
    def _(q):
        start_own(q)

    def arrive(q, part):
        y_copy(q, part).wait_recv()

        @pl.when(forwards)
        def _():
            x_copy(q, part, 2).start()

    arrive(0, 0)
    arrive(0, 1)

    @pl.loop(0, chunks)
    def _(q):
        for side in range(2):
            column = column_of(q, k if side == 0 else 1 - k)
            lanes = pl.ds(side * LANES, LANES)
            factors = vec[0, :, pl.ds(pl.multiple_of(q * wide + side * LANES, LANES), LANES)]

            @pl.loop(0, rows // block)
            def _(b):
                at = pl.ds(pl.multiple_of(b * block, block), block)
                scaled = (buf[0, q, at, lanes].astype(jnp.float32) * factors[0:1, :]).astype(jnp.bfloat16)
                own_t[pl.ds(column, LANES), at] = scaled.T

            back[pl.ds(column, LANES), :] = jnp.broadcast_to(factors[1:2, :], (LANES, LANES)).T

    def swap_copy(m, g):
        return pltpu.make_async_remote_copy(
            swap_out.at[m % 2, rows_of(g)], swap_in.at[m % swap_slots, rows_of(g)],
            swap_send.at[m % 2, g], swap_recv.at[m % swap_slots, g],
            device_id=(c, 2 * z + 1 - k), device_id_type=MESH_ID)

    def near_copy(m, g):
        return pltpu.make_async_remote_copy(
            line.at[m % line_slots, rows_of(g)], near.at[near_slot(m), rows_of(g)],
            line_send.at[m % line_slots, g], near_recv.at[near_slot(m), g],
            device_id=(c, partner), device_id_type=MESH_ID)

    def far_copy(m, offset, q, g):
        slot = offset * parts + q // pairs
        return pltpu.make_async_remote_copy(
            line.at[m % line_slots, rows_of(g)], far.at[slot, rows_of(g)],
            line_send.at[m % line_slots, g], far_recv.at[slot, g],
            device_id=(c, 2 * target_of(q) + k), device_id_type=MESH_ID)

    def out_copy(m, offset, q, g):
        lanes = pl.ds(pl.multiple_of((q // pairs) * LANES, LANES), LANES)
        return pltpu.make_async_copy(
            hold.at[m % hold_slots, rows_of(g)], out.at[offset, rows_of(g), lanes],
            out_sem.at[m % hold_slots, g])

    def turn_copy(part, g, core):
        return pltpu.make_async_remote_copy(
            turned.at[part, g, core], mirror.at[z - 1, k, part],
            turn_send.at[part, g, core], turn_recv.at[z - 1, k, part],
            device_id=(c, 2 * g + core), device_id_type=MESH_ID)

    def turn_arrival(goal, core, part):
        return pltpu.make_async_remote_copy(
            turned.at[0, 0, 0], mirror.at[goal - 1, core, part],
            turn_send.at[0, 0, 0], turn_recv.at[goal - 1, core, part],
            device_id=(c, 2 * goal + core), device_id_type=MESH_ID)

    def stage_copy(e, start):
        return pltpu.make_async_copy(
            stage.at[e % 2], out.at[0, pl.ds(start, LANES), :], stage_sem.at[e % 2])

    def mirrored(e):
        goal, core, part = e // (2 * parts) + 1, (e // parts) % 2, e % parts
        start = pl.multiple_of((2 * goal + core) * piece + part * LANES, LANES)
        return goal, core, part, start

    @pl.loop(0, last + hold_slots)
    def _(n):
        def settle(m, action):
            offset, q = stage_of(m)

            @pl.when(valid(m))
            def _():
                @pl.loop(0, blocks_of(offset, q))
                def _(g):
                    action(offset, q, g)

        def close_swap(offset, q, g):
            swap_copy(n - 2, g).wait_send()

        def close_out(offset, q, g):
            @pl.when(role_of(q) == 3)
            def _():
                out_copy(n - hold_slots, offset, q, g).wait()

        def close_line(offset, q, g):
            @pl.when(role_of(q) != 3)
            def _():
                near_copy(n - 1 - line_slots, g).wait_send()

        settle(n - 2, close_swap)
        settle(n - hold_slots, close_out)

        turn = n // 3

        @pl.when((n % 3 == 1) & (turn > 0) & (turn < chunks))
        def _():
            arrive(turn, 1)

        @pl.when((n % 3 == 2) & (turn < chunks))
        def _():
            arrive(turn, 3)

        @pl.when(n == 2)
        def _():
            vec_copy(2).wait_recv()

        @pl.when(n == 4)
        def _():
            vec_copy(1).wait_recv()

        @pl.when(valid(n))
        def _():
            offset, q = stage_of(n)

            @pl.when(offset == 1)
            def _():
                for part in range(pieces):
                    x_copy(q, part, 0).wait_recv()

            factors = vec[offset, 0:1, pl.ds(pl.multiple_of(q * wide, wide), wide)]

            @pl.loop(0, rows // block)
            def _(b):
                at = pl.ds(pl.multiple_of(b * block, block), block)
                chunk[at, :] = (buf[offset, q, at, :].astype(jnp.float32) * factors).astype(jnp.bfloat16)

        settle(n - 1 - line_slots, close_line)

        def join(offset, q, g):
            m = n - 1
            at = rows_of(g)
            role = role_of(q)
            swap_copy(m, g).wait_recv()

            @pl.when(role == 1)
            def _():
                line[m % line_slots, at, :] = sent(hold[m % hold_slots, at, :] + swap_in[m % swap_slots, at, :])

                @pl.when((g == 0) & (m >= near_slots) & valid(m - near_slots) & (m != near_slots + 1))
                def _():
                    pl.semaphore_wait(near_free.at[m % near_slots], 1)

                near_copy(m, g).start()

            @pl.when(role != 1)
            def _():
                hold[m % hold_slots, at, :] = hold[m % hold_slots, at, :] + swap_in[m % swap_slots, at, :]

        settle(n - 1, join)

        @pl.when((n % 3 == 0) & (turn > 0) & (turn < chunks))
        def _():
            arrive(turn, 0)

        @pl.when((n % 3 == 1) & (turn < chunks))
        def _():
            arrive(turn, 2)

        def multiply(offset, q, g):
            at = rows_of(g)
            product = jnp.dot(own_t[at, :], chunk[...], preferred_element_type=jnp.float32)
            hold[n % hold_slots, at, :] = product[:, :LANES]
            swap_out[n % 2, at, :] = product[:, LANES:]
            swap_copy(n, g).start()

        settle(n, multiply)

        def give_back(m, offset, q, g):
            @pl.when((g == blocks_of(offset, q) - 1) & valid(m + near_slots) & (m != 1))
            def _():
                pl.semaphore_signal(
                    near_free.at[m % near_slots], inc=1, device_id=(c, partner), device_id_type=MESH_ID)

        def relay(offset, q, g):
            m = n - 3
            at = rows_of(g)

            @pl.when(role_of(q) == 2)
            def _():
                near_copy(m, g).wait_recv()
                line[m % line_slots, at, :] = sent(
                    hold[m % hold_slots, at, :] + received(near[near_slot(m), at, :]))
                give_back(m, offset, q, g)
                far_copy(m, offset, q, g).start()

        settle(n - 3, relay)

        def finish(offset, q, g):
            m = n - 6
            at = rows_of(g)

            @pl.when(role_of(q) == 3)
            def _():
                near_copy(m, g).wait_recv()
                far_copy(m, offset, q, g).wait_recv()
                part = q // pairs
                factors = vec[offset, 1:2, pl.ds(pl.multiple_of(q * wide, wide), LANES)]
                total = hold[m % hold_slots, at, :] + received(near[near_slot(m), at, :])
                total = total + received(far[offset * parts + part, at, :])
                hold[m % hold_slots, at, :] = total * back[at, :] * factors
                give_back(m, offset, q, g)
                out_copy(m, offset, q, g).start()

                @pl.when((offset == 0) & (g < z))
                def _():
                    across = sent(total).T
                    for core in range(2):
                        turned[part, g, core] = across[:, core * piece:(core + 1) * piece]
                        turn_copy(part, g, core).start()

        settle(n - 6, finish)

        @pl.when(n == last + 1)
        def _():
            factors = plain[1:2, pl.ds(pl.multiple_of(r * piece, piece), piece)]

            @pl.loop(2 * parts * z, 2 * parts * (pairs - 1))
            def _(e):
                goal, core, part, start = mirrored(e)
                turn_arrival(goal, core, part).wait_recv()

                @pl.when(e >= 2 * parts * z + 2)
                def _():
                    stage_copy(e - 2, mirrored(e - 2)[3]).wait()

                sizes = back[pl.ds(start, LANES), :]
                sizes = jnp.concatenate([sizes] * (piece // LANES), axis=1)
                stage[e % 2] = received(mirror[goal - 1, core, part]) * sizes * factors
                stage_copy(e, start).start()

    @pl.when(z < pairs - 1)
    def _():
        for e in range(2 * parts * (pairs - 1) - 2, 2 * parts * (pairs - 1)):
            stage_copy(e, mirrored(e)[3]).wait()

    @pl.loop(0, z)
    def _(g):
        for part in range(parts):
            for core in range(2):
                turn_copy(part, g, core).wait_send()

    @pl.loop(0, chunks)
    def _(q):
        for part in range(pieces):
            y_copy(q, part).wait_send()
            x_copy(q, part, 0).wait_send()

    for step in range(1, n_row):
        sum_copy(step).wait_send()
    for offset in (2, 1):
        vec_copy(offset).wait_send()


def square_program(n_row):
    def on_device(data, column_scale, keep_mask):
        rows, panel = data.shape
        piece = panel // n_row
        pairs, parts = n_row // 2, piece // LANES
        chunks = pairs * parts
        f32, bf16, dma = jnp.float32, jnp.bfloat16, pltpu.SemaphoreType.DMA
        band = pl.pallas_call(
            functools.partial(square_kernel, n_row),
            out_shape=jax.ShapeDtypeStruct((3, panel, piece), f32),
            in_specs=[pl.BlockSpec(memory_space=pl.ANY), pl.BlockSpec(memory_space=pltpu.VMEM),
                      pl.BlockSpec(memory_space=pl.ANY)],
            out_specs=pl.BlockSpec(memory_space=pl.ANY),
            scratch_shapes=[
                pltpu.VMEM((3, chunks, rows, 2 * LANES), bf16),
                pltpu.VMEM((panel, rows), bf16),
                pltpu.VMEM((rows, 2 * LANES), bf16),
                pltpu.VMEM((2, panel, LANES), f32),
                pltpu.VMEM((3, panel, LANES), f32),
                pltpu.VMEM((7, panel, LANES), f32),
                pltpu.VMEM((3 * pairs + 1, panel, LANES), bf16),
                pltpu.VMEM((3 * parts, panel, LANES), bf16),
                pltpu.VMEM((5, panel, LANES), bf16),
                pltpu.VMEM((parts, pairs - 1, 2, LANES, piece), bf16),
                pltpu.VMEM((pairs - 1, 2, parts, LANES, piece), bf16),
                pltpu.VMEM((2, LANES, piece), f32),
                pltpu.VMEM((3, rows, LANES), jnp.int32),
                pltpu.VMEM((n_row, 1, panel), f32),
                pltpu.VMEM((8, panel), f32),
                pltpu.VMEM((3, 8, panel), f32),
                pltpu.VMEM((panel, LANES), f32),
                dma((2 * chunks,)), dma((4,)), dma((n_row,)), dma((n_row,)), dma((3,)), dma((3,)),
                dma((chunks, 4)), dma((chunks, 4)), dma((chunks, 4)), dma((chunks, 4)),
                dma((2, pairs)), dma((3, pairs)), dma((5, pairs)), dma((3 * pairs + 1, pairs)),
                dma((3 * parts, pairs)), dma((parts, pairs - 1, 2)), dma((pairs - 1, 2, parts)),
                dma((7, pairs)), dma((2,)), pltpu.SemaphoreType.REGULAR((3 * pairs,)),
            ],
            compiler_params=pltpu.CompilerParams(
                collective_id=0, has_side_effects=True, vmem_limit_bytes=67_043_328),
        )(data, column_scale[None, :], keep_mask)
        return band.transpose(1, 0, 2)

    return on_device


def solution(mesh):
    in_specs = (P("row", "col"), P("col"), P("row", "col"))
    out_specs = P("col", None, "row")

    def mapped(body):
        return jax.shard_map(
            body, mesh=mesh, in_specs=in_specs, out_specs=out_specs, check_vma=False
        )

    if mesh.shape["col"] == 4 and mesh.shape["row"] == 8:
        return mapped(square_program(mesh.shape["row"]))
    return mapped(on_device)
```

```python
import functools

import jax
import jax.numpy as jnp
from jax import lax
from jax.experimental import pallas as pl
from jax.experimental.pallas import tpu as pltpu
from jax.experimental.layout import Layout, with_layout_constraint
from jax.sharding import PartitionSpec as P


CHUNKS = 2
TOP = 16384.0


def passed_along(block, axis, distance):
    size = lax.axis_size(axis)
    return lax.ppermute(block, axis, [((i - distance) % size, i) for i in range(size)])


def swapped(block, axis):
    return lax.ppermute(block, axis, [(i, i ^ 1) for i in range(lax.axis_size(axis))])


def product(left, right):
    return lax.dot_general(
        left, right, (((0,), (0,)), ((), ())), preferred_element_type=jnp.float32
    )


def chunk_of(block, owners, q):
    width = block.shape[-1] // (owners * CHUNKS)
    starts = [(owner * CHUNKS + q) * width for owner in range(owners)]
    return jnp.concatenate([block[..., s:s + width] for s in starts], axis=-1)


def summed_over_rows(partial, pairs):
    me = lax.axis_index("row")
    pair, half = me // 2, me % 2
    parts = partial.reshape((pairs, 2, -1) + partial.shape[1:])
    mine = lax.dynamic_index_in_dim(parts, half, 1, keepdims=False)
    theirs = lax.dynamic_index_in_dim(parts, 1 - half, 1, keepdims=False)
    from_partner = swapped(theirs, "row")

    def both(at):
        one, two = (
            lax.dynamic_index_in_dim(a, at % pairs, 0, keepdims=False).astype(jnp.float32)
            for a in (mine, from_partner)
        )
        return one + two

    total = both(pair)
    plain = Layout(major_to_minor=(0, 1))
    blocks = [
        with_layout_constraint(both(pair + step).astype(jnp.float16), plain)
        for step in range(1, pairs)
    ]
    for step, block in enumerate(blocks, 1):
        arrived = with_layout_constraint(passed_along(block, "row", 2 * step), plain)
        total = total + arrived.astype(jnp.float32)
    return total, blocks


def on_device(data, column_scale, keep_mask):
    rows = lax.axis_size("row")
    n_col = lax.axis_size("col")
    offsets = n_col // 2 + 1
    values = data.astype(jnp.float32) * column_scale[None, :]
    colsq = lax.psum(jnp.sum(values * values, axis=0), "row")
    total_rows = data.shape[0] * rows
    divisor = jnp.minimum(jnp.sqrt(colsq + 1.0), jnp.sqrt(jnp.float32(total_rows)))
    norm = jnp.sqrt(jnp.maximum(colsq, 1e-30)) / divisor
    norms = [norm] + [passed_along(norm, "col", -offset) for offset in range(1, offsets)]
    divisor, norms = lax.optimization_barrier((divisor, norms))
    scaled = (keep_mask.astype(jnp.float32) * values / divisor[None, :]).astype(jnp.bfloat16)
    even = lax.axis_index("col") % 2 == 0

    own = [chunk_of(scaled, rows, q) for q in range(CHUNKS)]
    panels = {(0, q): own[q] for q in range(CHUNKS)}
    for q in range(CHUNKS):
        for offset in range(2, offsets, 2):
            panels[offset, q] = passed_along(own[q], "col", -offset)
    gain = TOP / norm
    kept = {}

    def stage(name, panel, length):
        partial = product(panel, scaled) * gain[None, :] * (1.0 / length)[:, None]
        partial = partial.astype(jnp.float16)
        total, blocks = summed_over_rows(partial, rows // 2)
        back = length.reshape(rows, -1)[lax.axis_index("row")]
        kept[name] = total * (norm * (1.0 / TOP))[None, :] * back[:, None]
        return blocks

    blocks = stage("0", scaled, norm)
    for offset in list(range(2, offsets, 2)) + list(range(1, offsets, 2)):
        for q in range(CHUNKS):
            if offset % 2:
                if n_col % 2 == 0 and (offset + 1, q) in panels:
                    after, before = panels[offset + 1, q], panels[offset - 1, q]
                    panels[offset, q] = swapped(jnp.where(even, after, before), "col")
                else:
                    panels[offset, q] = passed_along(own[q], "col", -offset)
            panels[offset, q], blocks = lax.optimization_barrier((panels[offset, q], blocks))
            length = chunk_of(norms[offset], rows, q)
            blocks = stage(f"{offset}_{q}", panels[offset, q], length)
    result = [kept["0"]]
    for offset in range(1, offsets):
        result.append(jnp.concatenate([kept[f"{offset}_{q}"] for q in range(CHUNKS)], axis=0))
    return jnp.stack([total.T for total in result], axis=1)


LANES = 128
SENT_TOP = 1024.0
MESH_ID = pl.DeviceIdType.MESH


def sent(x):
    x = x * jnp.abs(x)
    return (x * jnp.abs(x)).astype(jnp.bfloat16)


def received(y):
    y = y.astype(jnp.float32)
    size = lax.rsqrt(lax.rsqrt(jnp.maximum(jnp.abs(y), 1e-37)))
    return jnp.where(y < 0.0, -size, size)


def square_kernel(
    n_row, data, scale, mask, out,
    buf, own_t, chunk, swap_out, swap_in, hold, near, far, line, turned, mirror, stage, masks, sums, plain, vec, back,
    data_sem, mask_sem, sum_send, sum_recv, vec_send, vec_recv, y_send, y_recv, x_send, x_recv,
    swap_send, swap_recv, line_send, near_recv, far_recv, turn_send, turn_recv, out_sem, stage_sem, near_free,
):
    c, r = lax.axis_index("col"), lax.axis_index("row")
    z, k = r // 2, r % 2
    rows, panel = data.shape
    pairs = n_row // 2
    piece = panel // n_row
    wide = 2 * LANES
    parts = piece // LANES
    chunks = pairs * parts
    block = rows // 4
    pieces = 4
    cut = rows // pieces
    last = 3 * chunks + 2
    near_slots, hold_slots, line_slots, swap_slots = 3 * pairs, 6, 5, 3
    tall = panel // pairs
    forwards = c % 2 == 0
    y_peer, x_peer = (c + 2) % 4, c + 1 - 2 * (c % 2)
    partner = 2 * (z + 1 - 2 * (z % 2)) + k
    inner = jnp.logical_or(z == 1, z == 2)

    def target_of(q):
        at = q % pairs
        return jnp.where(at == 0, 0, jnp.where(at == 1, 2, jnp.where(at == 2, 3, 1)))

    def column_of(q, core):
        start = (2 * target_of(q) + core) * piece + (q // pairs) * LANES
        return pl.multiple_of(start, LANES)

    def stage_of(m):
        offset, turn = m % 3, m // 3
        ahead = jnp.where(m == 1, 0, (turn + 1) % chunks)
        own = jnp.logical_or(m == 1, offset == 0)
        return jnp.where(own, 0, offset), jnp.where(own, ahead, turn - jnp.where(offset == 1, 1, 0))

    def valid(m):
        return (m >= 0) & (m < last) & (m != last - 5) & (m != last - 2)

    def near_slot(m):
        return jnp.where(m == 1, near_slots, m % near_slots)

    def blocks_of(offset, q):
        return jnp.where(offset == 0, target_of(q) + 1, pairs)

    def rows_of(g):
        return pl.ds(pl.multiple_of(g * tall, tall), tall)

    def role_of(q):
        goal = target_of(q)
        same = z // 2 == goal // 2
        return jnp.where(z == goal, 3, jnp.where(same, 1, jnp.where(inner, 2, 1)))

    ahead = 3

    def strip_of(u):
        q, side = u // 2, u % 2
        to = pl.ds(pl.multiple_of(side * LANES, LANES), LANES)
        return q, to, pl.ds(column_of(q, k + side - 2 * k * side), LANES)

    def data_copy(u):
        q, to, columns = strip_of(u)
        return pltpu.make_async_copy(data.at[:, columns], buf.at[0, q, :, to], data_sem.at[u])

    def mask_copy(u):
        _, _, columns = strip_of(u)
        return pltpu.make_async_copy(mask.at[:, columns], masks.at[u % ahead], mask_sem.at[u % ahead])

    def cut_of(offset, q, part):
        return buf.at[offset, q, pl.ds(part * cut, cut), :]

    def y_copy(q, part):
        return pltpu.make_async_remote_copy(
            cut_of(0, q, part), cut_of(2, q, part), y_send.at[q, part], y_recv.at[q, part],
            device_id=(y_peer, r), device_id_type=MESH_ID)

    def x_copy(q, part, source):
        return pltpu.make_async_remote_copy(
            cut_of(source, q, part), cut_of(1, q, part), x_send.at[q, part], x_recv.at[q, part],
            device_id=(x_peer, r), device_id_type=MESH_ID)

    def start_own(q):
        for part in range(pieces):
            y_copy(q, part).start()

            @pl.when(jnp.logical_not(forwards))
            def _():
                x_copy(q, part, 0).start()

    for u in range(ahead):
        data_copy(u).start()
        mask_copy(u).start()

    @pl.loop(ahead, 2 * chunks)
    def _(u):
        data_copy(u).start()

    barrier = pltpu.get_barrier_semaphore()
    for step in range(1, n_row):
        pl.semaphore_signal(barrier, inc=1, device_id=(c, (r + step) % n_row), device_id_type=MESH_ID)
    for step in range(1, 4):
        pl.semaphore_signal(barrier, inc=1, device_id=((c + step) % 4, r), device_id_type=MESH_ID)
    pl.semaphore_wait(barrier, n_row + 2)

    @pl.loop(0, 2 * chunks)
    def _(u):
        data_copy(u).wait()
        mask_copy(u).wait()
        q, to, columns = strip_of(u)
        step = 256

        def read(b, total):
            at = pl.ds(pl.multiple_of(b * step, step), step)
            values = buf[0, q, at, to].astype(jnp.float32)
            kept = masks[u % ahead, at, :].astype(jnp.float32) * values
            buf[0, q, at, to] = kept.astype(jnp.bfloat16)
            return total + jnp.sum((values * values).reshape(step // 8, 8, LANES), axis=0)

        total = lax.fori_loop(0, rows // step, read, jnp.zeros((8, LANES), jnp.float32))
        scales = scale[:, columns]
        sums[r, :, columns] = jnp.sum(total, axis=0, keepdims=True) * scales * scales

        @pl.when(u + ahead < 2 * chunks)
        def _():
            mask_copy(u + ahead).start()

        @pl.when(u == 1)
        def _():
            start_own(0)

    def sum_copy(step):
        peer = (r + step) % n_row
        return pltpu.make_async_remote_copy(
            sums.at[r], sums.at[r], sum_send.at[step], sum_recv.at[step],
            device_id=(c, peer), device_id_type=MESH_ID)

    def sum_arrival(step):
        origin = (r + n_row - step) % n_row
        return pltpu.make_async_remote_copy(
            sums.at[origin], sums.at[origin], sum_send.at[step], sum_recv.at[step],
            device_id=(c, origin), device_id_type=MESH_ID)

    for step in range(1, n_row):
        sum_copy(step).start()
    for step in range(1, n_row):
        sum_arrival(step).wait_recv()
    colsq = sums[0]
    for origin in range(1, n_row):
        colsq = colsq + sums[origin]
    divisor = jnp.minimum(jnp.sqrt(colsq + 1.0), jnp.sqrt(jnp.full_like(colsq, rows * n_row)))
    size = jnp.sqrt(jnp.maximum(colsq, 1e-30)) / divisor
    up = jnp.full_like(size, SENT_TOP)
    down = jnp.full_like(size, 1.0 / SENT_TOP)
    for power in (32, 16, 8, 4, 2, 1):
        small = size < 2.0 ** -power
        size = jnp.where(small, size * 2.0 ** power, size)
        up = jnp.where(small, up * 2.0 ** power, up)
        down = jnp.where(small, down * 2.0 ** -power, down)
    plain[0:1, :] = scale[...] / divisor * up
    plain[1:2, :] = down

    @pl.loop(0, chunks)
    def _(q):
        for side in range(2):
            column = column_of(q, k if side == 0 else 1 - k)
            to = pl.ds(pl.multiple_of(q * wide + side * LANES, LANES), LANES)
            vec[0, :, to] = plain[:, pl.ds(column, LANES)]

    def vec_copy(offset):
        return pltpu.make_async_remote_copy(
            vec.at[0], vec.at[offset], vec_send.at[offset], vec_recv.at[offset],
            device_id=((c + 4 - offset) % 4, r), device_id_type=MESH_ID)

    for offset in (2, 1):
        vec_copy(offset).start()

    @pl.loop(1, chunks)
    def _(q):
        start_own(q)

    def arrive(q, part):
        y_copy(q, part).wait_recv()

        @pl.when(forwards)
        def _():
            x_copy(q, part, 2).start()

    arrive(0, 0)
    arrive(0, 1)

    @pl.loop(0, chunks)
    def _(q):
        for side in range(2):
            column = column_of(q, k if side == 0 else 1 - k)
            lanes = pl.ds(side * LANES, LANES)
            factors = vec[0, :, pl.ds(pl.multiple_of(q * wide + side * LANES, LANES), LANES)]

            @pl.loop(0, rows // block)
            def _(b):
                at = pl.ds(pl.multiple_of(b * block, block), block)
                scaled = (buf[0, q, at, lanes].astype(jnp.float32) * factors[0:1, :]).astype(jnp.bfloat16)
                own_t[pl.ds(column, LANES), at] = scaled.T

            back[pl.ds(column, LANES), :] = jnp.broadcast_to(factors[1:2, :], (LANES, LANES)).T

    def swap_copy(m, g):
        return pltpu.make_async_remote_copy(
            swap_out.at[m % 2, rows_of(g)], swap_in.at[m % swap_slots, rows_of(g)],
            swap_send.at[m % 2, g], swap_recv.at[m % swap_slots, g],
            device_id=(c, 2 * z + 1 - k), device_id_type=MESH_ID)

    def near_copy(m, g):
        return pltpu.make_async_remote_copy(
            line.at[m % line_slots, rows_of(g)], near.at[near_slot(m), rows_of(g)],
            line_send.at[m % line_slots, g], near_recv.at[near_slot(m), g],
            device_id=(c, partner), device_id_type=MESH_ID)

    def far_copy(m, offset, q, g):
        slot = offset * parts + q // pairs
        return pltpu.make_async_remote_copy(
            line.at[m % line_slots, rows_of(g)], far.at[slot, rows_of(g)],
            line_send.at[m % line_slots, g], far_recv.at[slot, g],
            device_id=(c, 2 * target_of(q) + k), device_id_type=MESH_ID)

    def out_copy(m, offset, q, g):
        lanes = pl.ds(pl.multiple_of((q // pairs) * LANES, LANES), LANES)
        return pltpu.make_async_copy(
            hold.at[m % hold_slots, rows_of(g)], out.at[offset, rows_of(g), lanes],
            out_sem.at[m % hold_slots, g])

    def turn_copy(part, g, core):
        return pltpu.make_async_remote_copy(
            turned.at[part, g, core], mirror.at[z - 1, k, part],
            turn_send.at[part, g, core], turn_recv.at[z - 1, k, part],
            device_id=(c, 2 * g + core), device_id_type=MESH_ID)

    def turn_arrival(goal, core, part):
        return pltpu.make_async_remote_copy(
            turned.at[0, 0, 0], mirror.at[goal - 1, core, part],
            turn_send.at[0, 0, 0], turn_recv.at[goal - 1, core, part],
            device_id=(c, 2 * goal + core), device_id_type=MESH_ID)

    def stage_copy(e, start):
        return pltpu.make_async_copy(
            stage.at[e % 2], out.at[0, pl.ds(start, LANES), :], stage_sem.at[e % 2])

    def mirrored(e):
        goal, core, part = e // (2 * parts) + 1, (e // parts) % 2, e % parts
        start = pl.multiple_of((2 * goal + core) * piece + part * LANES, LANES)
        return goal, core, part, start

    @pl.loop(0, last + hold_slots)
    def _(n):
        def settle(m, action):
            offset, q = stage_of(m)

            @pl.when(valid(m))
            def _():
                @pl.loop(0, blocks_of(offset, q))
                def _(g):
                    action(offset, q, g)

        def close_swap(offset, q, g):
            swap_copy(n - 2, g).wait_send()

        def close_out(offset, q, g):
            @pl.when(role_of(q) == 3)
            def _():
                out_copy(n - hold_slots, offset, q, g).wait()

        def close_line(offset, q, g):
            @pl.when(role_of(q) != 3)
            def _():
                near_copy(n - 1 - line_slots, g).wait_send()

        settle(n - 2, close_swap)
        settle(n - hold_slots, close_out)

        turn = n // 3

        @pl.when((n % 3 == 1) & (turn > 0) & (turn < chunks))
        def _():
            arrive(turn, 1)

        @pl.when((n % 3 == 2) & (turn < chunks))
        def _():
            arrive(turn, 3)

        @pl.when(n == 2)
        def _():
            vec_copy(2).wait_recv()

        @pl.when(n == 4)
        def _():
            vec_copy(1).wait_recv()

        @pl.when(valid(n))
        def _():
            offset, q = stage_of(n)

            @pl.when(offset == 1)
            def _():
                for part in range(pieces):
                    x_copy(q, part, 0).wait_recv()

            factors = vec[offset, 0:1, pl.ds(pl.multiple_of(q * wide, wide), wide)]

            @pl.loop(0, rows // block)
            def _(b):
                at = pl.ds(pl.multiple_of(b * block, block), block)
                chunk[at, :] = (buf[offset, q, at, :].astype(jnp.float32) * factors).astype(jnp.bfloat16)

        settle(n - 1 - line_slots, close_line)

        def join(offset, q, g):
            m = n - 1
            at = rows_of(g)
            role = role_of(q)
            swap_copy(m, g).wait_recv()

            @pl.when(role == 1)
            def _():
                line[m % line_slots, at, :] = sent(hold[m % hold_slots, at, :] + swap_in[m % swap_slots, at, :])

                @pl.when((g == 0) & (m >= near_slots) & valid(m - near_slots) & (m != near_slots + 1))
                def _():
                    pl.semaphore_wait(near_free.at[m % near_slots], 1)

                near_copy(m, g).start()

            @pl.when(role != 1)
            def _():
                hold[m % hold_slots, at, :] = hold[m % hold_slots, at, :] + swap_in[m % swap_slots, at, :]

        settle(n - 1, join)

        @pl.when((n % 3 == 0) & (turn > 0) & (turn < chunks))
        def _():
            arrive(turn, 0)

        @pl.when((n % 3 == 1) & (turn < chunks))
        def _():
            arrive(turn, 2)

        def multiply(offset, q, g):
            at = rows_of(g)
            product = jnp.dot(own_t[at, :], chunk[...], preferred_element_type=jnp.float32)
            hold[n % hold_slots, at, :] = product[:, :LANES]
            swap_out[n % 2, at, :] = product[:, LANES:]
            swap_copy(n, g).start()

        settle(n, multiply)

        def give_back(m, offset, q, g):
            @pl.when((g == blocks_of(offset, q) - 1) & valid(m + near_slots) & (m != 1))
            def _():
                pl.semaphore_signal(
                    near_free.at[m % near_slots], inc=1, device_id=(c, partner), device_id_type=MESH_ID)

        def relay(offset, q, g):
            m = n - 2
            at = rows_of(g)

            @pl.when(role_of(q) == 2)
            def _():
                near_copy(m, g).wait_recv()
                line[m % line_slots, at, :] = sent(
                    hold[m % hold_slots, at, :] + received(near[near_slot(m), at, :]))
                give_back(m, offset, q, g)
                far_copy(m, offset, q, g).start()

        settle(n - 2, relay)

        def finish(offset, q, g):
            m = n - 5
            at = rows_of(g)

            @pl.when(role_of(q) == 3)
            def _():
                near_copy(m, g).wait_recv()
                far_copy(m, offset, q, g).wait_recv()
                part = q // pairs
                factors = vec[offset, 1:2, pl.ds(pl.multiple_of(q * wide, wide), LANES)]
                total = hold[m % hold_slots, at, :] + received(near[near_slot(m), at, :])
                total = total + received(far[offset * parts + part, at, :])
                hold[m % hold_slots, at, :] = total * back[at, :] * factors
                give_back(m, offset, q, g)
                out_copy(m, offset, q, g).start()

                @pl.when((offset == 0) & (g < z))
                def _():
                    across = sent(total).T
                    for core in range(2):
                        turned[part, g, core] = across[:, core * piece:(core + 1) * piece]
                        turn_copy(part, g, core).start()

        settle(n - 5, finish)

        @pl.when(n == last + 1)
        def _():
            factors = plain[1:2, pl.ds(pl.multiple_of(r * piece, piece), piece)]

            @pl.loop(2 * parts * z, 2 * parts * (pairs - 1))
            def _(e):
                goal, core, part, start = mirrored(e)
                turn_arrival(goal, core, part).wait_recv()

                @pl.when(e >= 2 * parts * z + 2)
                def _():
                    stage_copy(e - 2, mirrored(e - 2)[3]).wait()

                sizes = back[pl.ds(start, LANES), :]
                sizes = jnp.concatenate([sizes] * (piece // LANES), axis=1)
                stage[e % 2] = received(mirror[goal - 1, core, part]) * sizes * factors
                stage_copy(e, start).start()

    @pl.when(z < pairs - 1)
    def _():
        for e in range(2 * parts * (pairs - 1) - 2, 2 * parts * (pairs - 1)):
            stage_copy(e, mirrored(e)[3]).wait()

    @pl.loop(0, z)
    def _(g):
        for part in range(parts):
            for core in range(2):
                turn_copy(part, g, core).wait_send()

    @pl.loop(0, chunks)
    def _(q):
        for part in range(pieces):
            y_copy(q, part).wait_send()
            x_copy(q, part, 0).wait_send()

    for step in range(1, n_row):
        sum_copy(step).wait_send()
    for offset in (2, 1):
        vec_copy(offset).wait_send()


def square_program(n_row):
    def on_device(data, column_scale, keep_mask):
        rows, panel = data.shape
        piece = panel // n_row
        pairs, parts = n_row // 2, piece // LANES
        chunks = pairs * parts
        f32, bf16, dma = jnp.float32, jnp.bfloat16, pltpu.SemaphoreType.DMA
        band = pl.pallas_call(
            functools.partial(square_kernel, n_row),
            out_shape=jax.ShapeDtypeStruct((3, panel, piece), f32),
            in_specs=[pl.BlockSpec(memory_space=pl.ANY), pl.BlockSpec(memory_space=pltpu.VMEM),
                      pl.BlockSpec(memory_space=pl.ANY)],
            out_specs=pl.BlockSpec(memory_space=pl.ANY),
            scratch_shapes=[
                pltpu.VMEM((3, chunks, rows, 2 * LANES), bf16),
                pltpu.VMEM((panel, rows), bf16),
                pltpu.VMEM((rows, 2 * LANES), bf16),
                pltpu.VMEM((2, panel, LANES), f32),
                pltpu.VMEM((3, panel, LANES), f32),
                pltpu.VMEM((6, panel, LANES), f32),
                pltpu.VMEM((3 * pairs + 1, panel, LANES), bf16),
                pltpu.VMEM((3 * parts, panel, LANES), bf16),
                pltpu.VMEM((5, panel, LANES), bf16),
                pltpu.VMEM((parts, pairs - 1, 2, LANES, piece), bf16),
                pltpu.VMEM((pairs - 1, 2, parts, LANES, piece), bf16),
                pltpu.VMEM((2, LANES, piece), f32),
                pltpu.VMEM((3, rows, LANES), jnp.int32),
                pltpu.VMEM((n_row, 1, panel), f32),
                pltpu.VMEM((8, panel), f32),
                pltpu.VMEM((3, 8, panel), f32),
                pltpu.VMEM((panel, LANES), f32),
                dma((2 * chunks,)), dma((4,)), dma((n_row,)), dma((n_row,)), dma((3,)), dma((3,)),
                dma((chunks, 4)), dma((chunks, 4)), dma((chunks, 4)), dma((chunks, 4)),
                dma((2, pairs)), dma((3, pairs)), dma((5, pairs)), dma((3 * pairs + 1, pairs)),
                dma((3 * parts, pairs)), dma((parts, pairs - 1, 2)), dma((pairs - 1, 2, parts)),
                dma((6, pairs)), dma((2,)), pltpu.SemaphoreType.REGULAR((3 * pairs,)),
            ],
            compiler_params=pltpu.CompilerParams(
                collective_id=0, has_side_effects=True, vmem_limit_bytes=67_043_328),
        )(data, column_scale[None, :], keep_mask)
        return band.transpose(1, 0, 2)

    return on_device


def solution(mesh):
    in_specs = (P("row", "col"), P("col"), P("row", "col"))
    out_specs = P("col", None, "row")

    def mapped(body):
        return jax.shard_map(
            body, mesh=mesh, in_specs=in_specs, out_specs=out_specs, check_vma=False
        )

    if mesh.shape["col"] == 4 and mesh.shape["row"] == 8:
        return mapped(square_program(mesh.shape["row"]))
    return mapped(on_device)
```
